256 devices in a mesh: groups: 2 (over z), expert: 16 (over x, core), tensor: 8 (over y).
Axes of the slice: x: 8, y: 8, z: 2, core: 2. Of those that a mesh axis runs over, the one named last changes fastest.
The devices are a block of a 8x8x16 slice.
Arguments:
- tokens: bfloat16 [2048, 4096], P(('groups', 'expert'), 'tensor'), parts along dimension 0, may hold values from -400 to 400
- norm_gain: float32 [4096], replicated, may hold values from 0.5 to 1.5
- w_gate: bfloat16 [4096, 65536], P(None, ('expert', 'tensor')), may hold values from -0.09375 to 0.09375
- w_up: bfloat16 [4096, 65536], P(None, ('expert', 'tensor')), may hold values from -0.09375 to 0.09375
- w_down: bfloat16 [65536, 4096], P(('expert', 'tensor')), may hold values from -0.0625 to 0.0625
- expert_ids: int32 [2048, 2], P(('groups', 'expert')), parts along dimension 0, may hold values from 0 to 7, all different within a row; in each aligned block of 64 rows (0 to 63, 64 to 127, ...) at most 32 rows name the same one
- gate_weights: float32 [2048, 2], P(('groups', 'expert')), parts along dimension 0, may hold values from 0.1 to 1
Outputs:
- moe_out: bfloat16 [2048, 4096], P(('groups', 'expert'), 'tensor'), parts along dimension 0
The draws below stay inside these ranges and needn't reach their ends.
There are 2 independent parts, one for each index of `groups`. The reference program is written for one: setup_inputs(seed, part) draws one part's arguments, and reference() takes and returns one part's arrays. A program takes and returns all parts, laid end to end along the dimension named above; an argument that names none is the same for every part. Nothing has to cross between parts.
Inputs may be any that keep to these rules, and one draw needn't show every extreme that they name: `expert_ids`: each request names two different experts. Within the rows of one device (aligned blocks of 64 rows) no expert is named by more than 32 rows, and in some blocks one expert is named by exactly 32 rows.
All inputs are finite; a program needn't handle non-finite values.
Results may differ from the reference program's by a relative error of at most 0.008.
Values may be sent and summed in bfloat16 or wider, within the bound.
No kernel may reach another device: no remote copies, remote signals or barrier semaphores. Data moves between devices by JAX's collectives and lax.ppermute only.
A program may use at most 128 MiB of HBM per device.

```python
import math
import jax
import jax.numpy as jnp
import numpy as np
from jax import lax

WIDTH = 4096
EXPERT_HIDDEN = 8192
EXPERTS = 8
TOK_DEV = 64
SLOTS = 32
TOKENS = 1024
N_EXPERT = 16


def draw_tokens(key, part):
    key_base, key_rows, key_cols = jax.random.split(key, 3)
    row_scale = jnp.exp(jax.random.uniform(key_rows, (TOKENS, 1), jnp.float32, 0.0, 2.3))
    ramp = jnp.exp(jnp.log(3.0) * jnp.arange(WIDTH, dtype=jnp.float32) / WIDTH)
    col_scale = ramp[None, :] * jnp.exp(jax.random.uniform(key_cols, (1, WIDTH), jnp.float32, -1.15, 1.15))
    base = jax.random.truncated_normal(key_base, -4.0, 4.0, (TOKENS, WIDTH), jnp.float32)
    return jnp.clip(base * row_scale * col_scale, -400.0, 400.0).astype(jnp.bfloat16)


def level_of(own_key, shape, shards, least, largest):
    gain, own = 1.0, jax.random.fold_in(own_key, 6)
    for dim, blocks in shards:
        draws = jnp.exp(jax.random.uniform(jax.random.fold_in(own, dim), (blocks,), jnp.float32, least / len(shards), largest / len(shards)))
        gain = gain * jnp.repeat(draws, shape[dim] // blocks).reshape([-1 if axis == dim else 1 for axis in range(len(shape))])
    return gain


def shared_out(stream_key, own, number, rows, amount, top, most, skew):
    sequence = jax.random.permutation(stream_key, amount)
    packed, usual = shares(amount, rows * top, most, skew, True), shares(amount, rows * top, most, skew, False)
    places = jnp.arange(amount)

    def named(sizes, turn):
        used = int((sizes > 0).sum())
        fixed = max(1, used // 4)
        shifted = fixed + (places - fixed + turn * (used - fixed)) % max(1, amount - fixed)
        return jnp.zeros((amount,), jnp.int32).at[sequence[jnp.where(places < fixed, places, shifted)]].set(jnp.asarray(sizes, jnp.int32))

    sizes = jnp.where(number % 4 == 0, named(packed, number // 4), named(usual, number - number // 4 - 1))
    mixed = jax.random.permutation(jax.random.fold_in(own, 3), amount)
    donor, receiver = mixed[0:amount // 2 * 2:2], mixed[1:amount // 2 * 2:2]
    room = jnp.minimum(sizes[donor] - 1, most - sizes[receiver]) // 2
    room = jnp.where((donor == sequence[0]) | (receiver == sequence[0]) | (sizes[receiver] == 0), 0, jnp.maximum(room, 0))
    shifted = jax.random.randint(jax.random.fold_in(own, 4), (amount // 2,), 0, 1 << 20) % (room + 1)
    sizes = sizes.at[donor].add(-shifted).at[receiver].add(shifted)
    members = jnp.searchsorted(jnp.cumsum(sizes), jnp.arange(rows * top), side="right").astype(jnp.int32)
    grid = members.reshape(top, rows).T
    grid = grid[jax.random.permutation(jax.random.fold_in(own, 1), rows)]
    turn = jax.random.randint(jax.random.fold_in(own, 2), (rows, 1), 0, top)
    return jnp.take_along_axis(grid, (jnp.arange(top)[None, :] + turn) % top, axis=1)


def shares(number_of, total, most, skew, full):
    weights = [(1 << 20) // math.isqrt(rank ** skew) + 1 for rank in range(1, number_of + 1)]
    largest = most if full else min(most, max(-(-total // number_of), total * weights[0] // sum(weights)))
    least = 1 if total - largest >= number_of - 1 else 0
    given, surplus = [largest] + [least] * (number_of - 1), total - largest - least * (number_of - 1)
    while surplus > 0:
        free = [i for i in range(1, number_of) if given[i] < largest] or [i for i in range(1, number_of) if given[i] < most]
        whole, remaining = sum([weights[i] for i in free]), surplus
        for i in free:
            more = min(most - given[i], max(1, remaining * weights[i] // whole), surplus)
            given[i] = given[i] + more
            surplus = surplus - more
    return np.array(given)


def scatter_about(stream_key, extent, deviation, reach, cuts=(), held_as=jnp.bfloat16):
    level = level_of(stream_key, extent, cuts, -0.22, 0.18) if cuts else 1.0
    values = jax.random.normal(stream_key, extent, jnp.float32) * deviation * level
    return jnp.minimum(jnp.maximum(values, -reach), reach).astype(held_as)


def setup_inputs(seed: int = 0, part: int = 0) -> dict:
    splits = jax.random.split(jax.random.key(seed), 8)
    part_splits = jax.random.split(jax.random.fold_in(splits[7], part), 8)
    tokens = draw_tokens(jax.random.fold_in(jax.random.fold_in(splits[7], part), 71), part)
    norm_gain = jnp.clip(1.0 + 0.1 * jax.random.normal(splits[1], (WIDTH,), jnp.float32), 0.5, 1.5)
    w_gate = scatter_about(splits[2], (WIDTH, EXPERTS * EXPERT_HIDDEN), WIDTH ** -0.5, 0.09375, ((1, 128),))
    w_up = scatter_about(splits[3], (WIDTH, EXPERTS * EXPERT_HIDDEN), WIDTH ** -0.5, 0.09375, ((1, 128),))
    w_down = scatter_about(splits[4], (EXPERTS * EXPERT_HIDDEN, WIDTH), EXPERT_HIDDEN ** -0.5, 0.0625, ((0, 128),))
    expert_ids_keys = jax.random.split(jax.random.fold_in(part_splits[5], 1), TOKENS // TOK_DEV)
    expert_ids_turns = jax.random.permutation(jax.random.fold_in(part_splits[5], 3), TOKENS // TOK_DEV)
    expert_ids = jax.vmap(lambda own, number: shared_out(jax.random.fold_in(part_splits[5], 2), own, number, TOK_DEV, EXPERTS, 2, SLOTS, 2))(expert_ids_keys, expert_ids_turns).reshape((TOKENS, 2))
    gate_weights = jnp.clip(0.1 + 0.9 * jax.random.uniform(part_splits[6], (TOKENS, 2), jnp.float32) ** level_of(part_splits[6], (TOKENS, 2), ((0, 16),), -0.2, 0.2), 0.1, 1.0)
    return {"tokens": tokens, "norm_gain": norm_gain, "w_gate": w_gate, "w_up": w_up, "w_down": w_down, "expert_ids": expert_ids, "gate_weights": gate_weights}


def reference(tokens, norm_gain, w_gate, w_up, w_down, expert_ids, gate_weights):
    values = tokens.astype(jnp.float32)
    mean_square = lax.optimization_barrier(jnp.mean(values * values, axis=1, keepdims=True))
    normed = (values * lax.rsqrt(mean_square + 1e-05) * norm_gain[None, :]).astype(jnp.bfloat16)
    capacity_all = N_EXPERT * SLOTS
    result = jnp.zeros((TOKENS, WIDTH), jnp.float32)
    for expert in range(EXPERTS):
        chosen = expert_ids == expert
        weight_of = lax.optimization_barrier(jnp.sum(jnp.where(chosen, gate_weights, jnp.zeros_like(gate_weights)), axis=1))
        is_routed = jnp.any(chosen, axis=1).astype(jnp.int32)
        picked = jnp.argsort(1 - is_routed, stable=True)[:capacity_all].astype(jnp.int32)
        row_data = jnp.take(normed, picked, axis=0)
        low = expert * EXPERT_HIDDEN
        high = low + EXPERT_HIDDEN
        gate_act = jnp.dot(row_data, w_gate[:, low:high], preferred_element_type=jnp.float32)
        up_act = jnp.dot(row_data, w_up[:, low:high], preferred_element_type=jnp.float32)
        hidden = (jax.nn.silu(gate_act) * up_act).astype(jnp.bfloat16)
        expert_out = jnp.dot(hidden, w_down[low:high, :], preferred_element_type=jnp.float32)
        weights_here = jnp.take(weight_of, picked, axis=0)
        result = result.at[picked].add(weights_here[:, None] * expert_out)
    return result.astype(jnp.bfloat16)
```

```python
import jax
import jax.numpy as jnp
from jax import lax
from jax.sharding import Mesh, PartitionSpec as P

EXPERTS = 8
CHUNKS = 1


def shift(value, axis, by):
    size = lax.axis_size(axis)
    return lax.ppermute(value, axis, [(i, (i + by) % size) for i in range(size)])


def place(whole, block, index, width):
    return lax.dynamic_update_slice(whole, block, (0, index * width))


def gather_features(chunks):
    n = lax.axis_size("tensor")
    me = lax.axis_index("tensor")
    rows, w = chunks[0].shape
    right, left = list(chunks), list(chunks)
    whole = [place(jnp.zeros((rows, n * w), c.dtype), c, me, w) for c in chunks]
    for step in range(1, n // 2 + 1):
        for i in range(len(chunks)):
            right[i] = shift(right[i], "tensor", 1)
            whole[i] = place(whole[i], right[i], (me - step) % n, w)
            if step < n - n // 2:
                left[i] = shift(left[i], "tensor", -1)
                whole[i] = place(whole[i], left[i], (me + step) % n, w)
    return whole


def sum_features(parts):
    n = lax.axis_size("tensor")
    me = lax.axis_index("tensor")
    w = parts[0].shape[1] // n

    def block(i, offset):
        return lax.dynamic_slice_in_dim(parts[i], ((me + offset) % n) * w, w, 1)

    right, left = [None] * len(parts), [None] * len(parts)
    far = n // 2
    for step in range(far):
        for i in range(len(parts)):
            value = block(i, far - step)
            if right[i] is not None:
                value = value + right[i].astype(jnp.float32)
            right[i] = shift(value.astype(jnp.bfloat16), "tensor", 1)
            if step < n - 1 - far:
                value = block(i, -(n - 1 - far - step))
                if left[i] is not None:
                    value = value + left[i].astype(jnp.float32)
                left[i] = shift(value.astype(jnp.bfloat16), "tensor", -1)
    return [
        block(i, 0) + right[i].astype(jnp.float32) + left[i].astype(jnp.float32)
        for i in range(len(parts))
    ]


def per_device(tokens, norm_gain, w_gate, w_up, w_down, expert_ids, gate_weights):
    columns, halves = lax.axis_size("column"), lax.axis_size("half")
    tok_rows, w = tokens.shape
    width = w * lax.axis_size("tensor")
    slots = tok_rows // 2
    share = slots // halves
    f32, bf16 = jnp.float32, jnp.bfloat16

    def swap(value):
        return [shift(value, "half", k) for k in range(1, halves)]

    gates, ups, downs = [w_gate] + swap(w_gate), [w_up] + swap(w_up), [w_down] + swap(w_down)

    experts = jnp.arange(EXPERTS, dtype=jnp.int32)
    hits = (expert_ids[:, :, None] == experts[None, None, :]).astype(f32)
    chosen = jnp.sum(hits, axis=1)
    order = jnp.arange(tok_rows, dtype=jnp.int32)
    earlier = (order[:, None] > order[None, :]).astype(bf16)
    rank = jnp.dot(earlier, chosen.astype(bf16), preferred_element_type=f32)
    slot = jnp.arange(slots, dtype=jnp.int32).astype(f32)
    select = chosen.T[:, None, :] * (rank.T[:, None, :] == slot[None, :, None]).astype(f32)
    weight = jnp.sum(hits * gate_weights[:, :, None], axis=1)

    pick = select.reshape(EXPERTS * slots, tok_rows).astype(bf16)
    packed = jnp.dot(pick, tokens, preferred_element_type=f32).astype(bf16)
    packed = packed.reshape(columns * halves, share, w)

    def to_experts(value):
        return lax.all_to_all(value, ("column", "half"), 0, 0, tiled=True)

    arrived = to_experts(packed).reshape(columns * halves * share, w)
    rows = arrived.shape[0] // CHUNKS
    whole = gather_features([arrived[i * rows : (i + 1) * rows] for i in range(CHUNKS)])

    def experts_of(x):
        values = x.astype(f32)
        mean_square = jnp.sum(values * values, axis=1, keepdims=True) / width
        normed = (values * lax.rsqrt(mean_square + 1e-05) * norm_gain[None, :]).astype(bf16)
        total = 0.0
        for gate, up, down in zip(gates, ups, downs):
            g = jnp.dot(normed, gate, preferred_element_type=f32)
            u = jnp.dot(normed, up, preferred_element_type=f32)
            hidden = (jax.nn.silu(g) * u).astype(bf16)
            total = total + jnp.dot(hidden, down, preferred_element_type=f32)
        return total

    summed = sum_features([experts_of(x) for x in whole])
    summed = jnp.concatenate(summed, axis=0).astype(bf16)
    returned = to_experts(summed.reshape(columns * halves, share, w)).reshape(EXPERTS * slots, w)
    mix = (select * weight.T[:, None, :]).reshape(EXPERTS * slots, tok_rows)
    mixed = lax.dot_general(
        mix,
        returned.astype(f32),
        (((0,), (0,)), ((), ())),
        precision=lax.Precision.HIGHEST,
        preferred_element_type=f32,
    )
    return mixed.astype(bf16)


def solution(mesh):
    groups, n_expert, n_tensor = (mesh.shape[a] for a in ("groups", "expert", "tensor"))
    halves = n_expert // EXPERTS
    inner = Mesh(
        mesh.devices.reshape(groups, EXPERTS, halves, n_tensor),
        ("groups", "column", "half", "tensor"),
    )
    rows = ("groups", "column", "half")
    hidden = ("column", "half", "tensor")
    in_specs = (
        P(rows, "tensor"),
        P(),
        P(None, hidden),
        P(None, hidden),
        P(hidden, None),
        P(rows, None),
        P(rows, None),
    )
    return jax.shard_map(
        per_device, mesh=inner, in_specs=in_specs, out_specs=P(rows, "tensor"), check_vma=False
    )
```

```python
import jax
import jax.numpy as jnp
from jax import lax
from jax.sharding import Mesh, PartitionSpec as P

EXPERTS = 8
CHUNKS = 1


def shift(value, axis, by):
    size = lax.axis_size(axis)
    return lax.ppermute(value, axis, [(i, (i + by) % size) for i in range(size)])


def block_of(value, index, size, axis):
    return lax.dynamic_slice_in_dim(value, index * size, size, axis)


def gather_features(chunks, use):
    n = lax.axis_size("tensor")
    me = lax.axis_index("tensor")
    right, left = list(chunks), list(chunks)
    for i, chunk in enumerate(chunks):
        use(i, chunk, me)
    for step in range(1, n // 2 + 1):
        for i in range(len(chunks)):
            with jax.named_scope(f"ag_r{step}_{i}"):
                right[i] = shift(right[i], "tensor", 1)
            if step < n - n // 2:
                with jax.named_scope(f"ag_l{step}_{i}"):
                    left[i] = shift(left[i], "tensor", -1)
            use(i, right[i], (me - step) % n)
            if step < n - n // 2:
                use(i, left[i], (me + step) % n)


def sum_features(make, count):
    n = lax.axis_size("tensor")
    me = lax.axis_index("tensor")
    right, left = [None] * count, [None] * count
    far = n // 2
    for step in range(far):
        for i in range(count):
            value = make(i, (me + far - step) % n)
            if right[i] is not None:
                value = value + right[i].astype(jnp.float32)
            with jax.named_scope(f"rs_r{step}_{i}"):
                right[i] = shift(value.astype(jnp.bfloat16), "tensor", 1)
            if step < n - 1 - far:
                value = make(i, (me - (n - 1 - far - step)) % n)
                if left[i] is not None:
                    value = value + left[i].astype(jnp.float32)
                with jax.named_scope(f"rs_l{step}_{i}"):
                    left[i] = shift(value.astype(jnp.bfloat16), "tensor", -1)
    return [
        make(i, me) + right[i].astype(jnp.float32) + left[i].astype(jnp.float32)
        for i in range(count)
    ]


def per_device(tokens, norm_gain, w_gate, w_up, w_down, expert_ids, gate_weights):
    columns, halves = lax.axis_size("column"), lax.axis_size("half")
    tok_rows, w = tokens.shape
    width = w * lax.axis_size("tensor")
    slots = tok_rows // 2
    share = slots // halves
    f32, bf16 = jnp.float32, jnp.bfloat16

    def swap(value):
        return [shift(value, "half", k) for k in range(1, halves)]

    gates, ups, downs = [w_gate] + swap(w_gate), [w_up] + swap(w_up), [w_down] + swap(w_down)

    experts = jnp.arange(EXPERTS, dtype=jnp.int32)
    hits = (expert_ids[:, :, None] == experts[None, None, :]).astype(f32)
    chosen = jnp.sum(hits, axis=1)
    order = jnp.arange(tok_rows, dtype=jnp.int32)
    earlier = (order[:, None] > order[None, :]).astype(bf16)
    rank = jnp.dot(earlier, chosen.astype(bf16), preferred_element_type=f32)
    slot = jnp.arange(slots, dtype=jnp.int32).astype(f32)
    select = chosen.T[:, None, :] * (rank.T[:, None, :] == slot[None, :, None]).astype(f32)
    weight = jnp.sum(hits * gate_weights[:, :, None], axis=1)

    pick = select.reshape(EXPERTS * slots, tok_rows).astype(bf16)
    packed = jnp.dot(pick, tokens, preferred_element_type=f32).astype(bf16)
    packed = packed.reshape(columns * halves, share, w)

    def to_experts(value):
        return lax.all_to_all(value, ("column", "half"), 0, 0, tiled=True)

    arrived = to_experts(packed).reshape(columns * halves * share, w)
    rows = arrived.shape[0] // CHUNKS
    gate_sums = [[0.0] * halves for _ in range(CHUNKS)]
    up_sums = [[0.0] * halves for _ in range(CHUNKS)]
    squares = [0.0] * CHUNKS

    def accumulate(i, block, owner):
        values = block.astype(f32)
        squares[i] = squares[i] + jnp.sum(values * values, axis=1, keepdims=True)
        scaled = (values * block_of(norm_gain, owner, w, 0)[None, :]).astype(bf16)
        for k in range(halves):
            gate, up = block_of(gates[k], owner, w, 0), block_of(ups[k], owner, w, 0)
            gate_sums[i][k] = gate_sums[i][k] + jnp.dot(scaled, gate, preferred_element_type=f32)
            up_sums[i][k] = up_sums[i][k] + jnp.dot(scaled, up, preferred_element_type=f32)

    gather_features([arrived[i * rows : (i + 1) * rows] for i in range(CHUNKS)], accumulate)
    hidden = []
    for i in range(CHUNKS):
        scale = lax.rsqrt(squares[i] / width + 1e-05)
        hidden.append(
            [
                (jax.nn.silu(g * scale) * (u * scale)).astype(bf16)
                for g, u in zip(gate_sums[i], up_sums[i])
            ]
        )

    def partial(i, owner):
        return sum(
            jnp.dot(h, block_of(down, owner, w, 1), preferred_element_type=f32)
            for h, down in zip(hidden[i], downs)
        )

    summed = sum_features(partial, CHUNKS)
    summed = jnp.concatenate(summed, axis=0).astype(bf16)
    returned = to_experts(summed.reshape(columns * halves, share, w)).reshape(EXPERTS * slots, w)
    mix = (select * weight.T[:, None, :]).reshape(EXPERTS * slots, tok_rows)
    mixed = lax.dot_general(
        mix,
        returned.astype(f32),
        (((0,), (0,)), ((), ())),
        precision=lax.Precision.HIGHEST,
        preferred_element_type=f32,
    )
    return mixed.astype(bf16)


def solution(mesh):
    groups, n_expert, n_tensor = (mesh.shape[a] for a in ("groups", "expert", "tensor"))
    halves = n_expert // EXPERTS
    inner = Mesh(
        mesh.devices.reshape(groups, EXPERTS, halves, n_tensor),
        ("groups", "column", "half", "tensor"),
    )
    rows = ("groups", "column", "half")
    hidden = ("column", "half", "tensor")
    in_specs = (
        P(rows, "tensor"),
        P(),
        P(None, hidden),
        P(None, hidden),
        P(hidden, None),
        P(rows, None),
        P(rows, None),
    )
    return jax.shard_map(
        per_device, mesh=inner, in_specs=in_specs, out_specs=P(rows, "tensor"), check_vma=False
    )
```

```python
import jax
import jax.numpy as jnp
from jax import lax
from jax.experimental import pallas as pl
from jax.experimental.pallas import tpu as pltpu
from jax.sharding import Mesh, PartitionSpec as P


EXPERTS = 8
CHUNKS = 1


def shift(value, axis, by):
    size = lax.axis_size(axis)
    return lax.ppermute(value, axis, [(i, (i + by) % size) for i in range(size)])


def hold_on_chip(*arrays):
    def kernel(*refs):
        count = len(arrays)
        sources, targets, done = refs[:count], refs[count : 2 * count], refs[2 * count]
        copies = [
            pltpu.make_async_copy(sources[k], targets[k], done.at[k]) for k in range(count)
        ]
        for copy in copies:
            copy.start()
        for copy in copies:
            copy.wait()

    return pl.pallas_call(
        kernel,
        out_shape=[pltpu.VMEM(a.shape, a.dtype) for a in arrays],
        in_specs=[pl.BlockSpec(memory_space=pl.ANY) for _ in arrays],
        out_specs=[pl.BlockSpec(memory_space=pltpu.VMEM) for _ in arrays],
        scratch_shapes=[pltpu.SemaphoreType.DMA((len(arrays),))],
        compiler_params=pltpu.CompilerParams(vmem_limit_bytes=1 << 20),
    )(*arrays)


def block_of(value, index, size, axis):
    return lax.dynamic_slice_in_dim(value, index * size, size, axis)


def gather_features(chunks, use):
    n = lax.axis_size("tensor")
    me = lax.axis_index("tensor")
    right, left = list(chunks), list(chunks)
    for i, chunk in enumerate(chunks):
        use(i, chunk, me)
    for step in range(1, n // 2 + 1):
        for i in range(len(chunks)):
            right[i] = shift(right[i], "tensor", 1)
            if step < n - n // 2:
                left[i] = shift(left[i], "tensor", -1)
            use(i, right[i], (me - step) % n)
            if step < n - n // 2:
                use(i, left[i], (me + step) % n)


def sum_features(make, count):
    n = lax.axis_size("tensor")
    me = lax.axis_index("tensor")
    right, left = [None] * count, [None] * count
    far = n // 2
    for step in range(far):
        for i in range(count):
            value = make(i, (me + far - step) % n)
            if right[i] is not None:
                value = value + right[i].astype(jnp.float32)
            right[i] = shift(value.astype(jnp.bfloat16), "tensor", 1)
            if step < n - 1 - far:
                value = make(i, (me - (n - 1 - far - step)) % n)
                if left[i] is not None:
                    value = value + left[i].astype(jnp.float32)
                left[i] = shift(value.astype(jnp.bfloat16), "tensor", -1)
    return [
        make(i, me) + right[i].astype(jnp.float32) + left[i].astype(jnp.float32)
        for i in range(count)
    ]


def per_device(tokens, norm_gain, w_gate, w_up, w_down, expert_ids, gate_weights):
    columns, halves = lax.axis_size("column"), lax.axis_size("half")
    tok_rows, w = tokens.shape
    width = w * lax.axis_size("tensor")
    slots = tok_rows // 2
    share = slots // halves
    f32, bf16 = jnp.float32, jnp.bfloat16

    def swap(value):
        return [value] + [shift(value, "half", k) for k in range(1, halves)]

    gates, ups, downs = swap(w_gate), swap(w_up), swap(w_down)
    for k in range(1, halves):
        gates[k], ups[k], downs[k] = hold_on_chip(gates[k], ups[k], downs[k])

    experts = jnp.arange(EXPERTS, dtype=jnp.int32)
    hits = (expert_ids[:, :, None] == experts[None, None, :]).astype(f32)
    chosen = jnp.sum(hits, axis=1)
    order = jnp.arange(tok_rows, dtype=jnp.int32)
    earlier = (order[:, None] > order[None, :]).astype(bf16)
    rank = jnp.dot(earlier, chosen.astype(bf16), preferred_element_type=f32)
    slot = jnp.arange(slots, dtype=jnp.int32).astype(f32)
    select = chosen.T[:, None, :] * (rank.T[:, None, :] == slot[None, :, None]).astype(f32)
    weight = jnp.sum(hits * gate_weights[:, :, None], axis=1)

    pick = select.reshape(EXPERTS * slots, tok_rows).astype(bf16)
    packed = jnp.dot(pick, tokens, preferred_element_type=f32).astype(bf16)
    packed = packed.reshape(columns * halves, share, w)

    def exchange(value):
        return lax.all_to_all(value, ("column", "half"), 0, 0, tiled=True)

    arrived = exchange(packed).reshape(columns * halves * share, w)
    rows = arrived.shape[0] // CHUNKS
    gate_sums = [[0.0] * halves for _ in range(CHUNKS)]
    up_sums = [[0.0] * halves for _ in range(CHUNKS)]
    squares = [0.0] * CHUNKS

    def accumulate(i, block, owner):
        values = block.astype(f32)
        squares[i] = squares[i] + jnp.sum(values * values, axis=1, keepdims=True)
        scaled = (values * block_of(norm_gain, owner, w, 0)[None, :]).astype(bf16)
        for k in range(halves):
            gate, up = block_of(gates[k], owner, w, 0), block_of(ups[k], owner, w, 0)
            gate_sums[i][k] = gate_sums[i][k] + jnp.dot(scaled, gate, preferred_element_type=f32)
            up_sums[i][k] = up_sums[i][k] + jnp.dot(scaled, up, preferred_element_type=f32)

    gather_features([arrived[i * rows : (i + 1) * rows] for i in range(CHUNKS)], accumulate)
    hidden = []
    for i in range(CHUNKS):
        scale = lax.rsqrt(squares[i] / width + 1e-05)
        hidden.append(
            [
                (jax.nn.silu(g * scale) * (u * scale)).astype(bf16)
                for g, u in zip(gate_sums[i], up_sums[i])
            ]
        )

    def partial(i, owner):
        return sum(
            jnp.dot(h, block_of(down, owner, w, 1), preferred_element_type=f32)
            for h, down in zip(hidden[i], downs)
        )

    summed = sum_features(partial, CHUNKS)
    summed = jnp.concatenate(summed, axis=0).astype(bf16)
    returned = exchange(summed.reshape(columns * halves, share, w))
    returned = returned.reshape(EXPERTS * slots, w)
    mix = (select * weight.T[:, None, :]).reshape(EXPERTS * slots, tok_rows)
    mixed = lax.dot_general(
        mix,
        returned.astype(f32),
        (((0,), (0,)), ((), ())),
        precision=lax.Precision.HIGHEST,
        preferred_element_type=f32,
    )
    return mixed.astype(bf16)


def solution(mesh):
    groups, n_expert, n_tensor = (mesh.shape[a] for a in ("groups", "expert", "tensor"))
    halves = n_expert // EXPERTS
    inner = Mesh(
        mesh.devices.reshape(groups, EXPERTS, halves, n_tensor),
        ("groups", "column", "half", "tensor"),
    )
    rows = ("groups", "column", "half")
    hidden = ("column", "half", "tensor")
    in_specs = (
        P(rows, "tensor"),
        P(),
        P(None, hidden),
        P(None, hidden),
        P(hidden, None),
        P(rows, None),
        P(rows, None),
    )

    return jax.shard_map(
        per_device, mesh=inner, in_specs=in_specs, out_specs=P(rows, "tensor"), check_vma=False
    )
```

```python
import jax
import jax.numpy as jnp
from jax import lax
from jax.experimental import pallas as pl
from jax.experimental.pallas import tpu as pltpu
from jax.sharding import Mesh, PartitionSpec as P


EXPERTS = 8


def shift(value, axis, by):
    size = lax.axis_size(axis)
    return lax.ppermute(value, axis, [(i, (i + by) % size) for i in range(size)])


def hold_on_chip(*arrays):
    def kernel(*refs):
        count = len(arrays)
        sources, targets, done = refs[:count], refs[count : 2 * count], refs[2 * count]
        copies = [
            pltpu.make_async_copy(sources[k], targets[k], done.at[k]) for k in range(count)
        ]
        for copy in copies:
            copy.start()
        for copy in copies:
            copy.wait()

    return pl.pallas_call(
        kernel,
        out_shape=[pltpu.VMEM(a.shape, a.dtype) for a in arrays],
        in_specs=[pl.BlockSpec(memory_space=pl.ANY) for _ in arrays],
        out_specs=[pl.BlockSpec(memory_space=pltpu.VMEM) for _ in arrays],
        scratch_shapes=[pltpu.SemaphoreType.DMA((len(arrays),))],
        compiler_params=pltpu.CompilerParams(vmem_limit_bytes=1 << 20),
    )(*arrays)


def block_of(value, index, size, axis):
    return lax.dynamic_slice_in_dim(value, index * size, size, axis)


class Pairs:
    def __init__(self):
        self.size, self.halves = lax.axis_size("tensor"), lax.axis_size("half")
        self.turn = lax.axis_index("half") % 2
        self.place = (lax.axis_index("tensor") + self.turn) % self.size
        self.steps = self.size // 2

    def partner(self, place, step):
        if step % 2:
            return place ^ 1
        return (place + (1 if place % 2 else -1)) % self.size

    def swap(self, value, step):
        n = self.size
        route = [
            (h * n + y, h * n + (self.partner((y + h % 2) % n, step) - h % 2) % n)
            for h in range(self.halves)
            for y in range(n)
        ]
        return lax.ppermute(value, ("half", "tensor"), route)

    def owners(self, step):
        base = self.place - self.place % 2
        away = 2 * (step // 2) * (-1) ** (step + 1)
        base = base + jnp.where(self.place % 2 == 0, away, -away)
        return [(base + k - self.turn) % self.size for k in range(2)]


def gather_features(chunk, use):
    pairs = Pairs()
    odd = pairs.place % 2 == 1
    use(chunk, lax.axis_index("tensor"))
    other = pairs.swap(chunk, 1)
    first, second = pairs.owners(1)
    use(other, jnp.where(odd, first, second))
    latest = jnp.where(odd, jnp.stack([other, chunk]), jnp.stack([chunk, other]))
    for step in range(2, pairs.steps + 1):
        latest = pairs.swap(latest, step)
        for k, owner in enumerate(pairs.owners(step)):
            use(latest[k], owner)


def sum_features(make):
    pairs = Pairs()
    f32, bf16 = jnp.float32, jnp.bfloat16
    came = None
    for step in range(pairs.steps, 1, -1):
        values = lax.optimization_barrier([make(owner) for owner in pairs.owners(step)])
        if came is not None:
            values = [value + came[k].astype(f32) for k, value in enumerate(values)]
        sent = jnp.stack([value.astype(bf16) for value in values])
        came = pairs.swap(sent, step)
    me = lax.axis_index("tensor")
    odd = pairs.place % 2 == 1
    first, second = pairs.owners(1)
    mine, other = lax.optimization_barrier((make(me), make(jnp.where(odd, first, second))))
    mine = mine + jnp.where(odd, came[1], came[0]).astype(f32)
    other = other + jnp.where(odd, came[0], came[1]).astype(f32)
    other = pairs.swap(other.astype(bf16), 1)
    return mine + other.astype(f32)


def per_device(tokens, norm_gain, w_gate, w_up, w_down, expert_ids, gate_weights):
    columns, halves = lax.axis_size("column"), lax.axis_size("half")
    tok_rows, w = tokens.shape
    width = w * lax.axis_size("tensor")
    slots = tok_rows // 2
    share = slots // halves
    f32, bf16 = jnp.float32, jnp.bfloat16

    def swap(value):
        return [value] + [shift(value, "half", k) for k in range(1, halves)]

    gates, ups, downs = swap(w_gate), swap(w_up), swap(w_down)
    for k in range(1, halves):
        gates[k], ups[k], downs[k] = hold_on_chip(gates[k], ups[k], downs[k])

    experts = jnp.arange(EXPERTS, dtype=jnp.int32)
    hits = (expert_ids[:, :, None] == experts[None, None, :]).astype(f32)
    chosen = jnp.sum(hits, axis=1)
    order = jnp.arange(tok_rows, dtype=jnp.int32)
    earlier = (order[:, None] > order[None, :]).astype(bf16)
    rank = jnp.dot(earlier, chosen.astype(bf16), preferred_element_type=f32)
    slot = jnp.arange(slots, dtype=jnp.int32).astype(f32)
    select = chosen.T[:, None, :] * (rank.T[:, None, :] == slot[None, :, None]).astype(f32)
    weight = jnp.sum(hits * gate_weights[:, :, None], axis=1)

    pick = select.reshape(EXPERTS * slots, tok_rows).astype(bf16)
    packed = jnp.dot(pick, tokens, preferred_element_type=f32).astype(bf16)
    packed = packed.reshape(columns * halves, share, w)

    def exchange(value):
        return lax.all_to_all(value, ("column", "half"), 0, 0, tiled=True)

    arrived = exchange(packed).reshape(columns * halves * share, w)
    gate_sums, up_sums, squares = [0.0] * halves, [0.0] * halves, [0.0]

    def accumulate(block, owner):
        values = block.astype(f32)
        squares[0] = squares[0] + jnp.sum(values * values, axis=1, keepdims=True)
        scaled = (values * block_of(norm_gain, owner, w, 0)[None, :]).astype(bf16)
        for k in range(halves):
            gate, up = block_of(gates[k], owner, w, 0), block_of(ups[k], owner, w, 0)
            gate_sums[k] = gate_sums[k] + jnp.dot(scaled, gate, preferred_element_type=f32)
            up_sums[k] = up_sums[k] + jnp.dot(scaled, up, preferred_element_type=f32)

    gather_features(arrived, accumulate)
    scale = lax.rsqrt(squares[0] / width + 1e-05)
    hidden = [
        (jax.nn.silu(g * scale) * (u * scale)).astype(bf16) for g, u in zip(gate_sums, up_sums)
    ]

    def partial(owner):
        return sum(
            jnp.dot(h, block_of(down, owner, w, 1), preferred_element_type=f32)
            for h, down in zip(hidden, downs)
        )

    summed = sum_features(partial).astype(bf16)
    returned = exchange(summed.reshape(columns * halves, share, w))
    returned = returned.reshape(EXPERTS * slots, w)
    mix = (select * weight.T[:, None, :]).reshape(EXPERTS * slots, tok_rows)
    mixed = lax.dot_general(
        mix,
        returned.astype(f32),
        (((0,), (0,)), ((), ())),
        precision=lax.Precision.HIGHEST,
        preferred_element_type=f32,
    )
    return mixed.astype(bf16)


def solution(mesh):
    groups, n_expert, n_tensor = (mesh.shape[a] for a in ("groups", "expert", "tensor"))
    halves = n_expert // EXPERTS
    inner = Mesh(
        mesh.devices.reshape(groups, EXPERTS, halves, n_tensor),
        ("groups", "column", "half", "tensor"),
    )
    rows = ("groups", "column", "half")
    hidden = ("column", "half", "tensor")
    in_specs = (
        P(rows, "tensor"),
        P(),
        P(None, hidden),
        P(None, hidden),
        P(hidden, None),
        P(rows, None),
        P(rows, None),
    )

    return jax.shard_map(per_device, mesh=inner, in_specs=in_specs, out_specs=P(rows, "tensor"), check_vma=False)
```
